256 devices in a mesh: af: 4 (over y), sa: 64 (over z, x, core).
Axes of the slice: x: 4, y: 4, z: 8, core: 2. Of those that a mesh axis runs over, the one named last changes fastest.
Arguments:
- data_real: bfloat16 [64, 512, 512], P('af', 'sa'), may hold values from -0.5 to 0.5
- data_imaginary: bfloat16 [64, 512, 512], P('af', 'sa'), may hold values from -0.5 to 0.5
- wavelet_real: float32 [64], P('af'), may hold values from -2.5 to 2.5
- wavelet_imaginary: float32 [64], P('af'), may hold values from -2.5 to 2.5
- primaries_real: float32 [64, 512, 512], P('af', 'sa'), may hold values from -3 to 3
- primaries_imaginary: float32 [64, 512, 512], P('af', 'sa'), may hold values from -3 to 3
Outputs:
- updated_real: float32 [64, 512, 512], P('af', 'sa')
- updated_imaginary: float32 [64, 512, 512], P('af', 'sa')
- misfit: float32 [2], replicated
The draws below stay inside these ranges and needn't reach their ends.
All inputs are finite; a program needn't handle non-finite values.
Results may differ from the reference program's by a relative error of at most 0.0018.
Values may be sent and summed in bfloat16 or wider, within the bound.
A program may use at most 64 MiB of HBM per device.

```python
import jax
import jax.numpy as jnp
from jax import lax

N = 512
F = 64
ITERS = 2


def levels(own_key, dims, cuts, low, top_value):
    gain, own = 1.0, jax.random.fold_in(own_key, 6)
    for axis_at, parts in cuts:
        steps = jnp.exp(jax.random.uniform(jax.random.fold_in(own, axis_at), (parts,), jnp.float32, low / len(cuts), top_value / len(cuts)))
        gain = gain * jnp.repeat(steps, dims[axis_at] // parts).reshape([-1 if axis == axis_at else 1 for axis in range(len(dims))])
    return gain


def scatter_about(rng, shape, deviation, most, pieces=(), kind=jnp.bfloat16):
    gain = levels(rng, shape, pieces, -0.22, 0.18) if pieces else 1.0
    result = jax.random.normal(rng, shape, jnp.float32) * deviation * gain
    return jnp.minimum(jnp.maximum(result, -most), most).astype(kind)


def setup_inputs(seed: int = 0) -> dict:
    streams_of = jax.random.split(jax.random.key(seed), 7)
    data_real = scatter_about(streams_of[0], (F, N, N), (N // 4) ** -0.5, 0.5, ((0, 4), (1, 64)))
    data_imaginary = scatter_about(streams_of[1], (F, N, N), (N // 4) ** -0.5, 0.5, ((0, 4), (1, 64)))
    wavelet_real = scatter_about(streams_of[2], (F,), 0.7, 2.5, ((0, 4),), jnp.float32)
    wavelet_imaginary = scatter_about(streams_of[3], (F,), 0.7, 2.5, ((0, 4),), jnp.float32)
    primaries_real = scatter_about(streams_of[4], (F, N, N), 0.5, 3.0, ((0, 4), (1, 64)), jnp.float32)
    primaries_imaginary = scatter_about(streams_of[5], (F, N, N), 0.5, 3.0, ((0, 4), (1, 64)), jnp.float32)
    return dict(data_real=data_real, data_imaginary=data_imaginary, wavelet_real=wavelet_real, wavelet_imaginary=wavelet_imaginary, primaries_real=primaries_real, primaries_imaginary=primaries_imaginary)


STEP_LENGTH = 0.02
THRESHOLD = 0.25


def forward_product(left, right):
    return jnp.einsum("frk,fkc->frc", left, right, precision=lax.Precision.HIGHEST)


def adjoint_product(left, right):
    return jnp.einsum("frk,fjk->frj", left, right, precision=lax.Precision.HIGHEST)


def rounded(values):
    return lax.optimization_barrier(values.astype(jnp.bfloat16)).astype(jnp.float32)


def reference(data_real, data_imaginary, wavelet_real, wavelet_imaginary, primaries_real, primaries_imaginary):
    slab_real = data_real.astype(jnp.float32)
    slab_imaginary = data_imaginary.astype(jnp.float32)
    wave_real = wavelet_real[:, None, None]
    wave_imaginary = wavelet_imaginary[:, None, None]
    current_real = primaries_real
    current_imaginary = primaries_imaginary
    misfits = []
    for iteration in range(ITERS):
        rounded_real = rounded(current_real)
        rounded_imaginary = rounded(current_imaginary)
        forward_real = forward_product(rounded_real, slab_real) - forward_product(rounded_imaginary, slab_imaginary)
        forward_imaginary = forward_product(rounded_real, slab_imaginary) + forward_product(rounded_imaginary, slab_real)
        error_real = slab_real + forward_real - (wave_real * current_real - wave_imaginary * current_imaginary)
        error_imaginary = slab_imaginary + forward_imaginary - (wave_real * current_imaginary + wave_imaginary * current_real)
        total = jnp.sum(error_real * error_real) + jnp.sum(error_imaginary * error_imaginary)
        misfits.append(total / (F * N * N))
        eb_real = rounded(error_real)
        eb_imaginary = rounded(error_imaginary)
        back_real = adjoint_product(eb_real, slab_real) + adjoint_product(eb_imaginary, slab_imaginary)
        back_imaginary = adjoint_product(eb_imaginary, slab_real) - adjoint_product(eb_real, slab_imaginary)
        gradient_real = wave_real * error_real + wave_imaginary * error_imaginary - back_real
        gradient_imaginary = wave_real * error_imaginary - wave_imaginary * error_real - back_imaginary
        stepped_real = current_real + STEP_LENGTH * gradient_real
        stepped_imaginary = current_imaginary + STEP_LENGTH * gradient_imaginary
        in_time = jnp.fft.ifft(stepped_real + 1j * stepped_imaginary, axis=0, norm="ortho")
        time_real = jnp.real(in_time)
        time_imaginary = jnp.imag(in_time)
        shrunk_real = time_real - jnp.clip(time_real, -THRESHOLD, THRESHOLD)
        shrunk_imaginary = time_imaginary - jnp.clip(time_imaginary, -THRESHOLD, THRESHOLD)
        in_frequency = jnp.fft.fft(shrunk_real + 1j * shrunk_imaginary, axis=0, norm="ortho")
        current_real = jnp.real(in_frequency).astype(jnp.float32)
        current_imaginary = jnp.imag(in_frequency).astype(jnp.float32)
    return current_real, current_imaginary, jnp.stack(misfits).astype(jnp.float32)
```

```python
import math

import jax
import jax.numpy as jnp
from jax import lax
from jax.experimental import pallas as pl
from jax.experimental.pallas import tpu as pltpu
from jax.sharding import Mesh
from jax.sharding import PartitionSpec as P

N = 512
F = 64
ITERS = 2
STEP_LENGTH = 0.02
THRESHOLD = 0.25

NY, NZ, NX, NC = 4, 8, 4, 2
NG = NX * NC
OWN = F // NY
ROWS = N // (NZ * NG)
ZROWS = ROWS * NG
COLS = N // NY
MESH = pl.DeviceIdType.MESH
SEND = jnp.bfloat16

PEERS_G = [(0, 1), (1, 0), (3, 0), (1, 1), (3, 1), (2, 0), (2, 1)]
CHUNKS = (
    ((0, 1, 3, 2), (0, 1, 3, 2), (0, 1, 3, 2), (0, 1)),
    ((0, 1, 3, 2), (1, 3, 0, 2), (3, 1, 2, 0), (3, 2)),
)
PAIR = 2 * ROWS
HOPS = [0, 1, 2, 1]
PEERS_T = sorted(
    [
        (dx, dc, dy)
        for dx in range(NX)
        for dc in range(NC)
        for dy in range(NY)
        if (dx, dc, dy) != (0, 0, 0)
    ],
    key=lambda p: -(2 * HOPS[p[0]] + 2 * HOPS[p[2]] + p[1]),
)


def dft8(v, sign):
    def add(p, q):
        return (p[0] + q[0], p[1] + q[1])

    def sub(p, q):
        return (p[0] - q[0], p[1] - q[1])

    def turn(p):
        return (-p[1], p[0]) if sign > 0 else (p[1], -p[0])

    def dft4(u):
        s0, s1 = add(u[0], u[2]), sub(u[0], u[2])
        s2, s3 = add(u[1], u[3]), turn(sub(u[1], u[3]))
        return add(s0, s2), add(s1, s3), sub(s0, s2), sub(s1, s3)

    a = [add(v[k], v[k + 4]) for k in range(4)]
    b = [sub(v[k], v[k + 4]) for k in range(4)]
    r = math.sqrt(0.5)
    t1, t3 = turn(b[1]), turn(b[3])
    b[1] = ((b[1][0] + t1[0]) * r, (b[1][1] + t1[1]) * r)
    b[2] = turn(b[2])
    b[3] = ((t3[0] - b[3][0]) * r, (t3[1] - b[3][1]) * r)
    even, odd = dft4(a), dft4(b)
    return [even[0], odd[0], even[1], odd[1], even[2], odd[2], even[3], odd[3]]


def encode(values, eighth):
    square = values * values
    signed = values * jnp.abs(values)
    if eighth:
        signed = signed * square * (square * square)
    else:
        signed = signed * square
    return signed.astype(SEND)


def decode(coded, eighth):
    coded = coded.astype(jnp.float32)
    root = lax.rsqrt(lax.rsqrt(jnp.abs(coded)))
    if eighth:
        root = root * lax.rsqrt(jnp.maximum(root, 1e-12))
    return jnp.where(coded < 0, -root, root)


def shrink(values):
    return values - jnp.clip(values, -THRESHOLD, THRESHOLD)


def kernel(
    dr, di, wave_real, wave_imaginary, pr, pi,
    outr, outi, mis,
    pin, turn, pbuf, flip, lbuf, fbuf, g0, g1, z0, z1, t0, t1, o0, o1, ubuf, wr, wi, mine_sums, tab, m1, m2,
    s_pin, s_own, s_px, r_px, s_g, r_g, s_ring, r_ring, s_t, r_t, l_t, s_c, r_c, l_c,
    s_o, r_o, l_o, s_m, r_m, s_w, ready, s_turn, r_turn,
):
    y, z = lax.axis_index("af"), lax.axis_index("z")
    x, c = lax.axis_index("x"), lax.axis_index("c")
    g = 2 * x + c
    xs = [lax.rem(x + d, NX) for d in range(NX)]
    cs = [c, 1 - c]
    ys = [lax.rem(y + d, NY) for d in range(NY)]
    zs = [lax.rem(z + d, NZ) for d in range(NZ)]
    gs = {(dx, dc): 2 * xs[dx] + cs[dc] for dx in range(NX) for dc in range(NC)}

    def total(ref, sem):
        pltpu.make_async_copy(ref, ref, sem).wait()

    copies = [
        pltpu.make_async_copy(dr, pin.at[0], s_pin.at[0]),
        pltpu.make_async_copy(di, pin.at[1], s_pin.at[1]),
    ]
    for copy in copies:
        copy.start()
    mine = pl.multiple_of(z * ZROWS + g * ROWS, ROWS)
    for part, ref in enumerate((dr, di)):
        pltpu.make_async_copy(
            ref.at[pl.ds(2 * g, 2)], pbuf.at[part, :, pl.ds(mine, ROWS), :], s_own.at[0]
        ).start()
    rows_g = pl.ds(pl.multiple_of(g * ROWS, ROWS), ROWS)
    for part, ref in enumerate((pr, pi)):
        pltpu.make_async_copy(
            ref.at[pl.ds(2 * g, 2)], g0.at[:, part, rows_g, :], s_own.at[1]
        ).start()

    with jax.named_scope("barrier"):
        barrier = pltpu.get_barrier_semaphore()
        for dx, dc in PEERS_G:
            pl.semaphore_signal(
                barrier, inc=1, device_id=(y, z, xs[dx], cs[dc]), device_id_type=MESH
            )
        for dy in (2, 1, 3):
            pl.semaphore_signal(barrier, inc=1, device_id=(ys[dy], z, x, c), device_id_type=MESH)
        for dz in (1, NZ - 1):
            for dc in range(2):
                pl.semaphore_signal(
                    barrier, inc=1, device_id=(y, zs[dz], x, cs[dc]), device_id_type=MESH
                )
        for b in range(8):
            for d in range(8):
                angle = 2.0 * math.pi * b * d / F
                tab[b * 8 + d] = jnp.float32(math.cos(angle) / 8.0)
                tab[64 + b * 8 + d] = jnp.float32(math.sin(angle) / 8.0)
        waves = [
            pltpu.make_async_copy(wave_real, wr, s_w.at[0]),
            pltpu.make_async_copy(wave_imaginary, wi, s_w.at[1]),
        ]
        for copy in waves:
            copy.start()
        pl.semaphore_wait(barrier, len(PEERS_G) + 7)
        for copy in copies:
            copy.wait()

    def send_rows(dx, dc):
        pltpu.make_async_remote_copy(
            src_ref=pin.at[:, pl.ds(2 * gs[dx, dc], 2)],
            dst_ref=pbuf.at[:, :, pl.ds(mine, ROWS), :],
            send_sem=s_px,
            recv_sem=r_px.at[2 * ((NX - dx) % NX) + dc],
            device_id=(y, z, xs[dx], cs[dc]),
            device_id_type=MESH,
        ).start()

    with jax.named_scope("xsends"):
        for dx, dc in PEERS_G[1:5]:
            send_rows(dx, dc)

    for dy in (2, 1, 3):
        pl.semaphore_signal(ready, inc=1, device_id=(ys[dy], z, x, c), device_id_type=MESH)

    def piece(block, first, rows, k):
        start = pl.multiple_of(block * ZROWS + first, ROWS)
        return pbuf.at[:, pl.ds(0, 2) if k is None else pl.ds(k, 1), pl.ds(start, rows), :]

    def hop(way, step, dx, k=None, dc=None):
        block = zs[(NZ - (step - 1)) % NZ] if way == 0 else zs[step - 1]
        if dc is None:
            ref = piece(block, PAIR * xs[dx], PAIR, k)
        else:
            ref = piece(block, ROWS * gs[dx, dc], ROWS, k)
        index = (step - 1) * 4 + (dx if step < 4 else 2 * k + dx % 2)
        pltpu.make_async_remote_copy(
            src_ref=ref,
            dst_ref=ref,
            send_sem=s_ring.at[way],
            recv_sem=r_ring.at[way, index],
            device_id=(y, zs[1] if way == 0 else zs[NZ - 1], x, c),
            device_id_type=MESH,
        ).start()

    def landed(way, step, dx, k=None):
        block = zs[(NZ - step) % NZ] if way == 0 else zs[step]
        index = (step - 1) * 4 + (dx if step < 4 else 2 * k + dx % 2)
        total(piece(block, PAIR * xs[dx], PAIR, k), r_ring.at[way, index])

    def arrived(dx, dc):
        total(piece(z, ROWS * gs[dx, dc], ROWS, None), r_px.at[2 * dx + dc])

    with jax.named_scope("zstart"):
        total(pbuf.at[:, :, pl.ds(0, ROWS), :], s_own.at[0])
        for way in range(2):
            hop(way, 1, 0, dc=0)
        for way, dz in enumerate((1, NZ - 1)):
            pltpu.make_async_remote_copy(
                src_ref=pin.at[:, pl.ds(2 * gs[0, 1], 2)],
                dst_ref=pbuf.at[:, :, pl.ds(mine, ROWS), :],
                send_sem=s_ring.at[way],
                recv_sem=r_ring.at[way, 0],
                device_id=(y, zs[dz], x, cs[1]),
                device_id_type=MESH,
            ).start()
        for dc in range(2):
            for way, dz in enumerate((1, NZ - 1)):
                pltpu.make_async_remote_copy(
                    src_ref=pin.at[:, pl.ds(2 * gs[2, dc], 2)],
                    dst_ref=turn.at[way, dc],
                    send_sem=s_ring.at[way],
                    recv_sem=r_turn.at[way, dc],
                    device_id=(y, zs[dz], x, c),
                    device_id_type=MESH,
                ).start()
    with jax.named_scope("xwait"):
        for dc in range(2):
            for dx in (1, 3):
                arrived(dx, dc)
                for way in range(2):
                    hop(way, 1, dx, dc=dc)
    with jax.named_scope("turn"):
        for dc in range(2):
            for way in range(2):
                total(turn.at[way, dc], r_turn.at[way, dc])
                block = zs[NZ - 1] if way == 0 else zs[1]
                pltpu.make_async_remote_copy(
                    src_ref=turn.at[way, dc],
                    dst_ref=piece(block, ROWS * g, ROWS, None),
                    send_sem=s_turn,
                    recv_sem=r_ring.at[way, 2],
                    device_id=(y, z, xs[2], cs[dc]),
                    device_id_type=MESH,
                ).start()

    for dx, dc in ((2, 0), (2, 1), (0, 1)):
        send_rows(dx, dc)

    def send_primaries():
        for dx, dc in PEERS_G:
            for part, ref in enumerate((pr, pi)):
                pltpu.make_async_remote_copy(
                    src_ref=ref.at[pl.ds(2 * gs[dx, dc], 2)],
                    dst_ref=g0.at[:, part, rows_g, :],
                    send_sem=s_g,
                    recv_sem=r_g,
                    device_id=(y, z, xs[dx], cs[dc]),
                    device_id_type=MESH,
                ).start()

    with jax.named_scope("ring"):
        for step in range(1, 4):
            if step == 2:
                send_primaries()
            here, sent = [set(), set()], [0, 0]
            for at in range(4):
                for way in range(2):
                    landed(way, step, CHUNKS[way][step - 1][at])
                    here[way].add(CHUNKS[way][step - 1][at])
                    order = [(dx, None) for dx in CHUNKS[way][step]]
                    if step == 3:
                        order = [(dx, k) for k in range(2) for dx in CHUNKS[way][step]]
                    while sent[way] < len(order) and order[sent[way]][0] in here[way]:
                        hop(way, step + 1, *order[sent[way]])
                        sent[way] += 1

    for dx, dc in ((0, 1), (2, 0), (2, 1)):
        arrived(dx, dc)
    total(g0.at[:, :, pl.ds(0, ROWS), :], s_own.at[1])
    total(g0.at[:, :, pl.ds(0, ROWS * (NG - 1)), :], r_g)

    last_pair = lax.rem(z + NZ // 2, NZ) // 2
    pair_rows = [
        pl.ds(pl.multiple_of(lax.rem(last_pair + i, NZ // 2) * 2 * ZROWS, 2 * ZROWS), 2 * ZROWS)
        for i in range(NZ // 2)
    ]

    def forward(k, part, rows):
        return jnp.dot(lbuf[k, :, rows], pbuf[part, k, rows, :], preferred_element_type=jnp.float32)

    with jax.named_scope("forward"):
        for k in range(2):
            for part in range(2):
                lbuf[k, pl.ds(part * ZROWS, ZROWS), :] = g0[k, part].astype(jnp.bfloat16)
            for part in range(2):
                fbuf[k, part] = sum(forward(k, part, rows) for rows in pair_rows[1:])
    for copy in waves:
        copy.wait()
    pl.semaphore_wait(ready, 3)

    columns = pl.ds(pl.multiple_of(y * COLS, COLS), COLS)
    own_rows = pl.ds(pl.multiple_of(z * ZROWS, ZROWS), ZROWS)

    def gradient_step(it, k, gbuf, zbuf):
        q_real, q_imaginary = wr[2 * g + k], wi[2 * g + k]
        real, imaginary = gbuf[k, 0], gbuf[k, 1]
        if it > 0:
            real, imaginary = decode(real, True), decode(imaginary, True)
        if it > 0:
            left = jnp.concatenate(
                [real.astype(jnp.bfloat16), imaginary.astype(jnp.bfloat16)], axis=0
            )
            with_real = jnp.dot(left, pbuf[0, k], preferred_element_type=jnp.float32)
            with_imaginary = jnp.dot(left, pbuf[1, k], preferred_element_type=jnp.float32)
        else:
            with_real = fbuf[k, 0] + forward(k, 0, pair_rows[0])
            with_imaginary = fbuf[k, 1] + forward(k, 1, pair_rows[0])
        error_real = (
            pbuf[0, k, own_rows, :].astype(jnp.float32)
            + (with_real[:ZROWS] - with_imaginary[ZROWS:])
            - (q_real * real - q_imaginary * imaginary)
        )
        error_imaginary = (
            pbuf[1, k, own_rows, :].astype(jnp.float32)
            + (with_imaginary[:ZROWS] + with_real[ZROWS:])
            - (q_real * imaginary + q_imaginary * real)
        )
        squares = error_real * error_real + error_imaginary * error_imaginary
        squares = jnp.sum(squares, axis=0, keepdims=True)
        squares = sum(squares[:, j * 128 : (j + 1) * 128] for j in range(N // 128))
        right = jnp.concatenate(
            [error_real.astype(jnp.bfloat16), error_imaginary.astype(jnp.bfloat16)], axis=0
        )
        if it == 0:
            across = (((1,), (1,)), ((), ()))
            with_real, with_imaginary = (
                lax.dot_general(right, pbuf[part, k], across, preferred_element_type=jnp.float32)
                for part in range(2)
            )
        else:
            with_real, with_imaginary = (
                jnp.dot(right, flip[part, k], preferred_element_type=jnp.float32)
                for part in range(2)
            )
        back_real = with_real[:ZROWS] + with_imaginary[ZROWS:]
        back_imaginary = with_real[ZROWS:] - with_imaginary[:ZROWS]
        step_real = q_real * error_real + q_imaginary * error_imaginary - back_real
        step_imaginary = q_real * error_imaginary - q_imaginary * error_real - back_imaginary
        zbuf[k, 0] = encode(real + STEP_LENGTH * step_real, it == 0)
        zbuf[k, 1] = encode(imaginary + STEP_LENGTH * step_imaginary, it == 0)
        return squares

    def to_time(it, k, zbuf, tbuf):
        slot = 16 * y + 2 * g + k
        for dx, dc, dy in PEERS_T:
            cut = zbuf.at[
                k,
                :,
                pl.ds(pl.multiple_of(gs[dx, dc] * ROWS, ROWS), ROWS),
                pl.ds(pl.multiple_of(ys[dy] * COLS, COLS), COLS),
            ]
            pltpu.make_async_remote_copy(
                src_ref=cut,
                dst_ref=tbuf.at[slot],
                send_sem=s_t.at[it],
                recv_sem=r_t.at[it, k],
                device_id=(ys[dy], z, xs[dx], cs[dc]),
                device_id_type=MESH,
            ).start()
        pltpu.make_async_copy(
            zbuf.at[k, :, rows_g, pl.ds(pl.multiple_of(y * COLS, COLS), COLS)],
            tbuf.at[slot],
            l_t.at[it, k],
        ).start()

    def first_pass(it, tbuf, b):
        v = [
            (decode(tbuf[8 * a + b, 0], it == 0), decode(tbuf[8 * a + b, 1], it == 0))
            for a in range(8)
        ]
        v = dft8(v, 1)
        for d in range(8):
            co, si = tab[b * 8 + d], tab[64 + b * 8 + d]
            ubuf[b * 8 + d, 0] = v[d][0] * co - v[d][1] * si
            ubuf[b * 8 + d, 1] = v[d][0] * si + v[d][1] * co

    def second_pass(d, carry):
        v = [(ubuf[b * 8 + d, 0], ubuf[b * 8 + d, 1]) for b in range(8)]
        v = [(shrink(p), shrink(q)) for p, q in dft8(v, 1)]
        v = dft8(v, -1)
        for b in range(8):
            co, si = tab[b * 8 + d], tab[64 + b * 8 + d]
            ubuf[b * 8 + d, 0] = v[b][0] * co + v[b][1] * si
            ubuf[b * 8 + d, 1] = v[b][1] * co - v[b][0] * si
        return carry

    def third_pass(it, obuf, b):
        v = [(ubuf[b * 8 + d, 0], ubuf[b * 8 + d, 1]) for d in range(8)]
        v = dft8(v, -1)
        for a in range(8):
            obuf[8 * a + b, 0] = encode(v[a][0], it == 0)
            obuf[8 * a + b, 1] = encode(v[a][1], it == 0)

    def time_side(it, tbuf, between):
        for k in range(2):
            with jax.named_scope("twait"):
                total(tbuf.at[pl.ds(0, 31)], r_t.at[it, k])
                total(tbuf.at[pl.ds(0, 1)], l_t.at[it, k])

            def at_b(j, carry, k=k):
                first_pass(it, tbuf, 2 * j + k)
                return carry

            with jax.named_scope("pass1"):
                lax.fori_loop(0, 4, at_b, 0, unroll=True)
        between()
        with jax.named_scope("pass2"):
            lax.fori_loop(0, 8, second_pass, 0, unroll=True)

    def share(m, stage, own, peers):
        for device in peers:
            pltpu.make_async_remote_copy(
                src_ref=m.at[own],
                dst_ref=m.at[own],
                send_sem=s_m.at[stage],
                recv_sem=r_m.at[stage],
                device_id=device,
                device_id_type=MESH,
            ).start()

    squares0 = jnp.zeros((1, 128), jnp.float32)
    for k in range(2):
        with jax.named_scope("ring4"):
            for at in range(2):
                for way in range(2):
                    landed(way, 4, CHUNKS[way][3][at], k)
        with jax.named_scope("grad"):
            squares0 = squares0 + gradient_step(0, k, g0, z0)
        with jax.named_scope("to_time"):
            to_time(0, k, z0, t0)
    with jax.named_scope("flip"):
        for k in range(2):
            for part in range(2):
                flip[part, k] = pbuf[part, k].T
    time_side(0, t0, lambda: None)
    with jax.named_scope("pass3_send"):
        for k in range(2):
            for px, dc in ((0, 1), (1, 1), (1, 0), (0, 0)):
                third_pass(0, o0, 2 * (2 * lax.rem(x + px, 2) + cs[dc]) + k)
                for dx in (px + 2, px):
                    for dy in (2, 1, 3, 0):
                        if (dx, dc, dy) == (0, 0, 0):
                            continue
                        pltpu.make_async_remote_copy(
                            src_ref=o0.at[16 * ys[dy] + 2 * gs[dx, dc] + k],
                            dst_ref=g1.at[k, :, rows_g, columns],
                            send_sem=s_c,
                            recv_sem=r_c.at[k],
                            device_id=(ys[dy], z, xs[dx], cs[dc]),
                            device_id_type=MESH,
                        ).start()
            pltpu.make_async_copy(
                o0.at[16 * y + 2 * g + k], g1.at[k, :, rows_g, columns], l_c.at[k]
            ).start()

    squares1 = jnp.zeros((1, 128), jnp.float32)
    for k in range(2):
        with jax.named_scope("cwait"):
            total(o0.at[pl.ds(0, 1)], l_c.at[k])
            total(o0.at[pl.ds(0, 31)], r_c.at[k])
        with jax.named_scope("grad"):
            squares1 = squares1 + gradient_step(1, k, g1, z1)
        if k == 1:
            m1[z] = jnp.concatenate([squares0, squares1], axis=0)
            share(m1, 0, z, [(y, zs[d], x, c) for d in (4, 3, 5, 2, 6, 1, 7)])
        with jax.named_scope("to_time"):
            to_time(1, k, z1, t1)

    member = NG * y + g

    def misfit_on():
        with jax.named_scope("misfit"):
            total(m1.at[pl.ds(0, NZ - 1)], r_m.at[0])
            m2[member] = sum(m1[i] for i in range(NZ))
            share(m2, 1, member, [(ys[dy], z, xs[dx], cs[dc]) for dx, dc, dy in PEERS_T])

    time_side(1, t1, misfit_on)
    with jax.named_scope("pass3"):
        for b in range(8):
            third_pass(1, o1, b)

    for dy in (2, 1, 3):
        for part, ref in enumerate((outr, outi)):
            pltpu.make_async_remote_copy(
                src_ref=o1.at[pl.ds(16 * ys[dy], 16), part],
                dst_ref=ref.at[:, :, columns],
                send_sem=s_o,
                recv_sem=r_o,
                device_id=(ys[dy], z, x, c),
                device_id_type=MESH,
            ).start()
    for part, ref in enumerate((outr, outi)):
        pltpu.make_async_copy(
            o1.at[pl.ds(16 * y, 16), part], ref.at[:, :, columns], l_o
        ).start()
    with jax.named_scope("sendwaits"):
        total(pbuf.at[:, :, pl.ds(0, ROWS * (NG - 1)), :], s_px)
        total(g0.at[:, :, pl.ds(0, ROWS * (NG - 1)), :], s_g)
        for way in range(2):
            total(pbuf.at[:, :, pl.ds(0, 3 * ZROWS), :], s_ring.at[way])
            total(pbuf.at[:, :, pl.ds(0, 2 * PAIR), :], s_ring.at[way])
        for it, tbuf in enumerate((t0, t1)):
            total(tbuf.at[pl.ds(0, 62)], s_t.at[it])
        total(turn, s_turn)
        total(o0.at[pl.ds(0, 62)], s_c)
        total(m1.at[pl.ds(0, NZ - 1)], s_m.at[0])
        total(m2.at[pl.ds(0, NY * NG - 1)], s_m.at[1])

    with jax.named_scope("mwait"):
        total(m2.at[pl.ds(0, NY * NG - 1)], r_m.at[1])
        sums = sum(m2[i] for i in range(NY * NG))
        for it in range(ITERS):
            mine_sums[it] = jnp.sum(sums[it : it + 1, :]) * (1.0 / (F * N * N))
        last = pltpu.make_async_copy(mine_sums, mis, s_w.at[0])
        last.start()

    with jax.named_scope("owait"):
        total(o1.at[pl.ds(0, 48)], s_o)
        total(o1.at[pl.ds(0, 48)], r_o)
        total(o1.at[pl.ds(0, 16)], l_o)
        last.wait()


def on_device(*arguments):
    hbm = pl.BlockSpec(memory_space=pltpu.HBM)
    anywhere = pl.BlockSpec(memory_space=pl.ANY)
    dma, f32 = pltpu.SemaphoreType.DMA, jnp.float32
    frequency_side = pltpu.VMEM((2, 2, ZROWS, N), SEND)
    time_side = pltpu.VMEM((F, 2, ROWS, COLS), SEND)
    out = jax.ShapeDtypeStruct((OWN, ROWS, N), SEND)
    real, imaginary, misfit = pl.pallas_call(
        kernel,
        out_shape=(out, out, jax.ShapeDtypeStruct((ITERS,), f32)),
        in_specs=[hbm] * 6,
        out_specs=(anywhere, anywhere, anywhere),
        scratch_shapes=[
            pltpu.VMEM((2, OWN, ROWS, N), jnp.bfloat16),
            pltpu.VMEM((2, 2, 2, 2, ROWS, N), jnp.bfloat16),
            pltpu.VMEM((2, 2, N, N), jnp.bfloat16),
            pltpu.VMEM((2, 2, N, N), jnp.bfloat16),
            pltpu.VMEM((2, 2 * ZROWS, N), jnp.bfloat16),
            pltpu.VMEM((2, 2, 2 * ZROWS, N), f32),
            pltpu.VMEM((2, 2, ZROWS, N), f32),
            frequency_side,
            frequency_side,
            frequency_side,
            time_side,
            time_side,
            time_side,
            time_side,
            pltpu.VMEM((F, 2, ROWS, COLS), f32),
            pltpu.SMEM((OWN,), f32),
            pltpu.SMEM((OWN,), f32),
            pltpu.SMEM((ITERS,), f32),
            pltpu.SMEM((2 * F,), f32),
            pltpu.VMEM((NZ, 2, 128), f32),
            pltpu.VMEM((NY * NG, 2, 128), f32),
            dma((2,)),
            dma((2,)),
            dma,
            dma((NG,)),
            dma,
            dma,
            dma((2,)),
            dma((2, 16)),
            dma((2,)),
            dma((2, 2)),
            dma((2, 2)),
            dma,
            dma((2,)),
            dma((2,)),
            dma,
            dma,
            dma,
            dma((2,)),
            dma((2,)),
            dma((2,)),
            pltpu.SemaphoreType.REGULAR,
            dma,
            dma((2, 2)),
        ],
        compiler_params=pltpu.CompilerParams(collective_id=0, has_side_effects=True, vmem_limit_bytes=24 * 2**20),
    )(*[pltpu.with_memory_space_constraint(a, pltpu.HBM) for a in arguments])
    return decode(real, False), decode(imaginary, False), misfit


def solution(mesh):
    split = Mesh(mesh.devices.reshape(NY, NZ, NX, NC), ("af", "z", "x", "c"))
    rows = P("af", ("z", "x", "c"), None)
    return jax.shard_map(
        on_device,
        mesh=split,
        in_specs=(rows, rows, P("af"), P("af"), rows, rows),
        out_specs=(rows, rows, P()),
        check_vma=False,
    )
```
